32 devices in a mesh: dp: 2 (over core), section: 4 (over z), mp: 4 (over y, x).
Axes of the slice: x: 2, y: 2, z: 4, core: 2. Of those that a mesh axis runs over, the one named last changes fastest.
Arguments:
- inputs: bfloat16 [48, 512], P(('dp', 'mp')), may hold values from -6 to 6
- tangents: bfloat16 [48, 32, 512], P(('dp', 'mp')), may hold values from -6 to 6
- targets: bfloat16 [48, 1024], P(('dp', 'mp')), may hold values from -24 to 24
- target_jac: bfloat16 [48, 32, 1024], P(('dp', 'mp')), may hold values from -24 to 24
- rank_mask: int32 [48, 32], P(('dp', 'mp')), may hold values from 0 to 1, as said below
- batch_order: int32 [8, 6], P(('dp', 'mp')), may hold values from 0 to 5, each once within a row
- encoder: bfloat16 [512, 2048], replicated, may hold values from -0.25 to 0.25
- layers: bfloat16 [4, 2048, 2048], P('section', 'mp'), may hold values from -0.125 to 0.125
- head_weight: bfloat16 [2048, 1024], replicated, may hold values from -0.125 to 0.125
Outputs:
- grad_layers: float32 [4, 2048, 2048], P('section', ('dp', 'mp'))
- grad_head: float32 [2048, 1024], P(('dp', 'mp'), 'section')
- loss_value: float32 [], replicated
The draws below stay inside these ranges and needn't reach their ends.
Inputs may be any that keep to these rules, and one draw needn't show every extreme that they name: `rank_mask`: each sample's ones are its first 1 to 32 directions. `batch_order`: each row is an ordering of 0 .. 5.
All inputs are finite; a program needn't handle non-finite values.
Results may differ from the reference program's by a relative error of at most 0.035.
Values may be sent and summed in bfloat16 or wider, within the bound.
A program may use at most 128 MiB of HBM per device.

```python
import jax
import jax.numpy as jnp
from jax import lax

D = 2048
DIN = 512
DOUT = 1024
RANK = 32
MB = 6
S_DEV = 1
SAMP_DEV = 6
GROUP_ROWS = 8
SAMPLES = 48
LAYERS = 4
N_DP = 2
N_MP = 4


def draw_rank_mask(key, part):
    jitter_key = jax.random.fold_in(key, 12)
    device_rows = jnp.arange(GROUP_ROWS, dtype=jnp.int32)[:, None]
    model_index = device_rows % N_MP
    base_rank = 1 + (RANK - 1) * model_index // max(N_MP - 1, 1)
    jitter = jax.random.randint(jitter_key, (GROUP_ROWS, SAMP_DEV), -1, 2)
    active = jnp.clip(base_rank + jitter, 1, RANK)
    last_row = jnp.arange(SAMP_DEV, dtype=jnp.int32)[None, :] == 0
    active = jnp.where((model_index == N_MP - 1) & last_row, RANK, active).reshape(SAMPLES, 1)
    return (jnp.arange(RANK, dtype=jnp.int32)[None, :] < active).astype(jnp.int32)


def row_scales(key):
    scale_key = jax.random.fold_in(key, 21)
    device_rows = jnp.arange(GROUP_ROWS, dtype=jnp.float32) / max(GROUP_ROWS - 1, 1)
    wobble = jax.random.uniform(scale_key, (GROUP_ROWS,), jnp.float32, -0.1, 0.1)
    low_end = jnp.log(0.3)
    high_end = jnp.log(3.9)
    return jnp.exp(low_end + (high_end - low_end) * device_rows + wobble)


def draw_targets(key, part):
    value_key = jax.random.fold_in(key, 22)
    scales = row_scales(key)[:, None, None]
    values = jnp.clip(jax.random.normal(value_key, (GROUP_ROWS, SAMP_DEV, DOUT), jnp.float32), -6.0, 6.0)
    return jnp.clip(scales * values, -24.0, 24.0).reshape(SAMPLES, DOUT).astype(jnp.bfloat16)


def draw_target_jac(key, part):
    value_key = jax.random.fold_in(key, 23)
    scales = row_scales(key)[:, None, None, None]
    shape = (GROUP_ROWS, SAMP_DEV, RANK, DOUT)
    values = jnp.clip(jax.random.normal(value_key, shape, jnp.float32), -6.0, 6.0)
    return jnp.clip(scales * values, -24.0, 24.0).reshape(SAMPLES, RANK, DOUT).astype(jnp.bfloat16)


def steps_of(own_key, extent, cuts, least, top_value):
    level, own = 1.0, jax.random.fold_in(own_key, 6)
    for axis_at, blocks in cuts:
        draws = jnp.exp(jax.random.uniform(jax.random.fold_in(own, axis_at), (blocks,), jnp.float32, least / len(cuts), top_value / len(cuts)))
        level = level * jnp.repeat(draws, extent[axis_at] // blocks).reshape([-1 if axis == axis_at else 1 for axis in range(len(extent))])
    return level


def normal_values(rng, shape, spread, limit, pieces=(), held_as=jnp.bfloat16):
    result = jax.random.normal(rng, shape, jnp.float32) * spread
    if len(pieces) > 0:
        result = steps_of(rng, shape, pieces, -0.22, 0.18) * result
    return jnp.clip(result, min=-limit, max=limit).astype(held_as)


def setup_inputs(seed: int = 0) -> dict:
    streams_of = jax.random.split(jax.random.key(seed), 10)
    return {
        "inputs": normal_values(streams_of[0], (SAMPLES, DIN), 1.0, 6.0, ((0, 8),)),
        "tangents": normal_values(streams_of[1], (SAMPLES, RANK, DIN), 1.0, 6.0, ((0, 8),)),
        "targets": draw_targets(jax.random.fold_in(streams_of[9], 71), 0),
        "target_jac": draw_target_jac(jax.random.fold_in(streams_of[9], 71), 0),
        "rank_mask": draw_rank_mask(jax.random.fold_in(streams_of[9], 71), 0),
        "batch_order": jax.vmap(lambda own: jax.random.permutation(own, SAMP_DEV))(jax.random.split(streams_of[5], GROUP_ROWS)).reshape((GROUP_ROWS, SAMP_DEV)).astype(jnp.int32),
        "encoder": normal_values(streams_of[6], (DIN, D), DIN ** -0.5, 0.25),
        "layers": normal_values(streams_of[7], (LAYERS, D, D), D ** -0.5, 0.125, ((0, 4), (1, 4))),
        "head_weight": normal_values(streams_of[8], (D, DOUT), D ** -0.5, 0.125),
    }


def forward_layer(row_block, weight):
    model_width = weight.shape[1]
    pre_act = jnp.dot(row_block.reshape(-1, model_width), weight, preferred_element_type=jnp.float32).reshape(row_block.shape)
    tanh_p = jnp.tanh(pre_act[:, 0])
    slope_vals = 1.0 - tanh_p * tanh_p
    primal = row_block[:, 0].astype(jnp.float32) + tanh_p
    tangent = row_block[:, 1:].astype(jnp.float32) + slope_vals[:, None, :] * pre_act[:, 1:]
    return jnp.concatenate([primal[:, None], tangent], axis=1).astype(jnp.bfloat16), pre_act


def backward_layer(row_block, pre_act, grad_rows, weight):
    model_width = weight.shape[1]
    upstream = grad_rows.astype(jnp.float32)
    tanh_p = jnp.tanh(pre_act[:, 0])
    slope_vals = 1.0 - tanh_p * tanh_p
    tangent_part = upstream[:, 1:] * slope_vals[:, None, :]
    slope_grad = jnp.sum(upstream[:, 1:] * pre_act[:, 1:], axis=1)
    primal_part = upstream[:, 0] * slope_vals - 2.0 * slope_grad * tanh_p * slope_vals
    grad_mix = jnp.concatenate([primal_part[:, None], tangent_part], axis=1).astype(jnp.bfloat16)
    back_rows = jnp.dot(grad_mix.reshape(-1, model_width), weight.T, preferred_element_type=jnp.float32).reshape(upstream.shape)
    return grad_mix, (upstream + back_rows).astype(jnp.bfloat16)


def block_sum(left, right):
    blocks = (left.reshape(N_DP * N_MP, -1, left.shape[-1]), right.reshape(N_DP * N_MP, -1, right.shape[-1]))

    def add_block(running, block_pair):
        partial_value = jnp.dot(block_pair[0].T, block_pair[1], preferred_element_type=jnp.float32)
        rounded = lax.optimization_barrier(partial_value.astype(jnp.bfloat16))
        return running + rounded.astype(jnp.float32), None

    running, _ = lax.scan(add_block, jnp.zeros((left.shape[-1], right.shape[-1]), jnp.float32), blocks)
    return running


def reference(inputs, tangents, targets, target_jac, rank_mask, batch_order, encoder, layers, head_weight):
    row_depth = RANK + 1
    rows_in = jnp.concatenate([inputs[:, None, :], tangents], axis=1)
    hidden = jnp.dot(rows_in.reshape(-1, DIN), encoder, preferred_element_type=jnp.float32).reshape(SAMPLES, row_depth, D).astype(jnp.bfloat16)
    saved_in = []
    saved_pre = []
    for layer_idx in range(LAYERS):
        saved_in.append(hidden)
        hidden, pre_act = forward_layer(hidden, layers[layer_idx])
        saved_pre.append(pre_act)
    outputs = jnp.dot(hidden.reshape(-1, D), head_weight, preferred_element_type=jnp.float32).reshape(SAMPLES, row_depth, DOUT)
    row_weight = jnp.concatenate([jnp.ones((SAMPLES, 1), jnp.float32), rank_mask.astype(jnp.float32)], axis=1)
    wanted = jnp.concatenate([targets[:, None, :], target_jac], axis=1).astype(jnp.float32)
    mismatch = outputs - wanted
    misfit = jnp.sum(row_weight[:, :, None] * mismatch * mismatch, axis=(1, 2))
    sample_index = (jnp.arange(GROUP_ROWS, dtype=jnp.int32)[:, None] * SAMP_DEV + batch_order).reshape(-1)
    batch_id = ((jnp.arange(GROUP_ROWS, dtype=jnp.int32)[:, None] // N_MP) * MB + (jnp.arange(SAMP_DEV, dtype=jnp.int32) // S_DEV)[None, :]).reshape(-1)
    micro_of = jnp.zeros((SAMPLES,), jnp.int32).at[sample_index].set(batch_id.astype(jnp.int32))
    totals = jax.ops.segment_sum(jnp.sum(row_weight, axis=1), micro_of, num_segments=N_DP * MB)
    divisor = totals[micro_of]
    loss_value = jnp.sum(misfit / divisor) / (N_DP * MB * DOUT)
    cot_out = (2.0 * row_weight[:, :, None] * mismatch / divisor[:, None, None]).astype(jnp.bfloat16)
    grad_head = block_sum(hidden, cot_out)
    grad_rows = jnp.dot(cot_out.reshape(-1, DOUT), head_weight.T, preferred_element_type=jnp.float32).reshape(SAMPLES, row_depth, D).astype(jnp.bfloat16)
    layer_grads = [None] * LAYERS
    for layer_idx in reversed(range(LAYERS)):
        grad_mix, grad_rows = backward_layer(saved_in[layer_idx], saved_pre[layer_idx], grad_rows, layers[layer_idx])
        layer_grads[layer_idx] = block_sum(saved_in[layer_idx], grad_mix)
    return jnp.stack(layer_grads), grad_head, loss_value
```

```python
import functools

import jax
import jax.numpy as jnp
from jax import lax
from jax.experimental import pallas as pl
from jax.experimental.pallas import tpu as pltpu
from jax.sharding import PartitionSpec as P

MB = 6


def from_behind(value, axis, steps):
    count = lax.axis_size(axis)
    initial, last = (max(0, -steps), min(count, count - steps))
    return lax.ppermute(value, axis, [(source, source + steps) for source in range(initial, last)])


def forward_layer(row_block, weight):
    model_width = weight.shape[1]
    pre_act = jnp.dot(
        row_block.reshape(-1, model_width), weight, preferred_element_type=jnp.float32
    ).reshape(row_block.shape)
    tanh_p = jnp.tanh(pre_act[:, 0])
    slope_vals = 1.0 - tanh_p * tanh_p
    primal = row_block[:, 0].astype(jnp.float32) + tanh_p
    tangent = row_block[:, 1:].astype(jnp.float32) + slope_vals[:, None, :] * pre_act[:, 1:]
    return (jnp.concatenate([primal[:, None], tangent], axis=1).astype(jnp.bfloat16), pre_act)


def backward_layer(pre_act, grad_rows, weight):
    model_width = weight.shape[1]
    upstream = grad_rows.astype(jnp.float32)
    tanh_p = jnp.tanh(pre_act[:, 0])
    slope_vals = 1.0 - tanh_p * tanh_p
    tangent_part = upstream[:, 1:] * slope_vals[:, None, :]
    slope_grad = jnp.sum(upstream[:, 1:] * pre_act[:, 1:], axis=1)
    primal_part = upstream[:, 0] * slope_vals - 2.0 * slope_grad * tanh_p * slope_vals
    grad_mix = jnp.concatenate([primal_part[:, None], tangent_part], axis=1).astype(jnp.bfloat16)
    back_rows = jnp.dot(
        grad_mix.reshape(-1, model_width), weight.T, preferred_element_type=jnp.float32
    ).reshape(upstream.shape)
    return (grad_mix, (upstream + back_rows).astype(jnp.bfloat16))


def place_slot(store, value, batch_slot, is_valid):
    return lax.dynamic_update_index_in_dim(
        store, jnp.where(is_valid, value, store[batch_slot]), batch_slot, 0
    )


def local(
    inputs, tangents, targets, target_jac, rank_mask, batch_order, encoder, layers, head_weight
):
    samp_dev = inputs.shape[0]
    per_batch = samp_dev // MB
    row_depth = tangents.shape[1] + 1
    in_width = inputs.shape[1]
    model_width = layers.shape[2]
    out_width = head_weight.shape[1]
    sections = lax.axis_size("section")
    section_id = lax.axis_index("section")
    is_first = section_id == 0
    is_last = section_id == sections - 1
    layer_full = lax.all_gather(layers[0], "mp", axis=0, tiled=True)
    sample_order = batch_order[0]
    row_weight = jnp.concatenate(
        [jnp.ones((samp_dev, 1), jnp.float32), rank_mask.astype(jnp.float32)], axis=1
    )
    sample_total = jnp.sum(row_weight, axis=1)
    batch_counts = lax.psum(
        jnp.sum(sample_total[sample_order].reshape(MB, per_batch), axis=1), "mp"
    )

    def picked_of(batch_slot):
        return lax.dynamic_slice_in_dim(sample_order, batch_slot * per_batch, per_batch)

    def lift_batch(batch_slot):
        picked = picked_of(batch_slot)
        rows_in = jnp.concatenate([inputs[picked][:, None, :], tangents[picked]], axis=1)
        lifted = jnp.dot(rows_in.reshape(-1, in_width), encoder, preferred_element_type=jnp.float32)
        return lifted.reshape(per_batch, row_depth, model_width).astype(jnp.bfloat16)

    block_shape = (MB, per_batch, row_depth, model_width)
    pre_shape = (1, 1, 1, 1)

    def forward_tick(step_index, loop_state):
        incoming, store_in, store_pre, store_out = loop_state
        batch_index = step_index - section_id
        is_valid = (batch_index >= 0) & (batch_index < MB)
        batch_slot = jnp.clip(batch_index, 0, MB - 1)
        row_block = lax.cond(is_first, lambda: lift_batch(batch_slot), lambda: incoming)

        def forward_active():
            return forward_layer(row_block, layer_full)

        def forward_resting():
            return (row_block, jnp.zeros(row_block.shape, jnp.float32))

        layer_out, pre_act = lax.cond(is_valid, forward_active, forward_resting)
        store_in = place_slot(store_in, row_block, batch_slot, is_valid)
        store_out = place_slot(store_out, layer_out, batch_slot, is_valid)
        passed = from_behind(layer_out, "section", 1)
        return (passed, store_in, store_pre, store_out)

    start_state = (
        jnp.zeros(block_shape[1:], jnp.bfloat16),
        jnp.zeros(block_shape, jnp.bfloat16),
        jnp.zeros(pre_shape, jnp.float32),
        jnp.zeros(block_shape, jnp.bfloat16),
    )
    _, store_in, store_pre, store_out = lax.fori_loop(
        0, MB + sections - 1, forward_tick, start_state
    )

    def backward_tick(step_index, loop_state):
        incoming, store_mix, store_head, loss_acc = loop_state
        batch_index = step_index - (sections - 1 - section_id)
        is_valid = (batch_index >= 0) & (batch_index < MB)
        batch_slot = jnp.clip(batch_index, 0, MB - 1)
        batch_total = batch_counts[batch_slot]

        def head_part():
            final_rows = store_out[batch_slot]
            outputs = jnp.dot(
                final_rows.reshape(-1, model_width), head_weight, preferred_element_type=jnp.float32
            )
            outputs = outputs.reshape(per_batch, row_depth, out_width)
            picked = picked_of(batch_slot)
            wanted = jnp.concatenate(
                [targets[picked][:, None, :], target_jac[picked]], axis=1
            ).astype(jnp.float32)
            weights_here = row_weight[picked]
            mismatch = outputs - wanted
            misfit = jnp.sum(weights_here[:, :, None] * mismatch * mismatch) / batch_total
            cot_out = (2.0 * weights_here[:, :, None] * mismatch / batch_total).astype(jnp.bfloat16)
            grad_rows = jnp.dot(
                cot_out.reshape(-1, out_width), head_weight.T, preferred_element_type=jnp.float32
            )
            return (
                grad_rows.reshape(per_batch, row_depth, model_width).astype(jnp.bfloat16),
                cot_out,
                misfit,
            )

        def pass_on():
            return (
                incoming,
                jnp.zeros((per_batch, row_depth, out_width), jnp.bfloat16),
                jnp.zeros((), jnp.float32),
            )

        grad_rows, cot_out, misfit = lax.cond(is_last & is_valid, head_part, pass_on)

        def backward_active():
            row_block = store_in[batch_slot]
            pre_act = jnp.dot(
                row_block.reshape(-1, model_width), layer_full, preferred_element_type=jnp.float32
            ).reshape(row_block.shape)
            return backward_layer(pre_act, grad_rows, layer_full)

        def backward_resting():
            return (jnp.zeros(grad_rows.shape, jnp.bfloat16), grad_rows)

        grad_mix, grad_in = lax.cond(is_valid, backward_active, backward_resting)
        store_mix = place_slot(store_mix, grad_mix, batch_slot, is_valid)
        store_head = place_slot(store_head, cot_out, batch_slot, is_valid)
        loss_acc = loss_acc + jnp.where(is_valid, misfit, jnp.zeros((), jnp.float32))
        passed = from_behind(grad_in, "section", -1)
        return (passed, store_mix, store_head, loss_acc)

    back_state = (
        jnp.zeros(block_shape[1:], jnp.bfloat16),
        jnp.zeros(block_shape, jnp.bfloat16),
        jnp.zeros((MB, per_batch, row_depth, out_width), jnp.bfloat16),
        jnp.zeros((), jnp.float32),
    )
    _, store_mix, store_head, loss_acc = lax.fori_loop(
        0, MB + sections - 1, backward_tick, back_state
    )
    shard_rows = model_width // (lax.axis_size("dp") * lax.axis_size("mp"))
    in_flat = store_in.reshape(-1, model_width)
    mix_flat = store_mix.reshape(-1, model_width)
    grad_layers = lax.psum_scatter(
        jnp.dot(in_flat.T, mix_flat, preferred_element_type=jnp.float32).astype(jnp.bfloat16),
        ("dp", "mp"),
        scatter_dimension=0,
        tiled=True,
    ).astype(jnp.float32)[None]
    out_flat = store_out.reshape(-1, model_width)
    head_flat = store_head.reshape(-1, out_width)

    def compute():
        return jnp.dot(out_flat.T, head_flat, preferred_element_type=jnp.float32)

    def skipped():
        return jnp.zeros((lax.axis_size(("dp", "mp")) * shard_rows, out_width), jnp.float32)

    summed = lax.psum_scatter(
        lax.cond(is_last, compute, skipped).astype(jnp.bfloat16),
        ("dp", "mp"),
        scatter_dimension=0,
        tiled=True,
    )
    section_loss = lax.psum(loss_acc, ("dp", "mp"))
    loss_row = jnp.broadcast_to(section_loss, (1, sections))
    grad_head, loss_cols = (
        lax.psum_scatter(summed, "section", scatter_dimension=1, tiled=True).astype(jnp.float32),
        lax.psum_scatter(
            loss_row.astype(jnp.bfloat16), "section", scatter_dimension=1, tiled=True
        ).astype(jnp.float32),
    )
    loss_value = loss_cols[0, 0] / (lax.axis_size("dp") * MB * out_width)
    return (grad_layers, grad_head, loss_value)


MESH = pl.DeviceIdType.MESH
TILE = 512
LANES = 128
SUBLANES = 16
PIECES = 4


def cuts_of(tang):
    weights = (2, 2, 1, 1)
    unit = tang // sum(weights)
    if unit % SUBLANES:
        return [(0, tang)]
    cuts, at = [], 0
    for weight in weights:
        cuts.append((at, at + weight * unit))
        at += weight * unit
    return cuts


def step_kernel(
    shape,
    shard_hbm, enc_hbm, head_hbm, tan_hbm, tjac_hbm, inp_ref, tgt_ref, mask_ref, order_ref,
    dw_ref, gh_ref, loss_ref,
    w, wt, enc, head, headt, tan, tjac, inp, tgt, hin, hout, pre, th, sacc, cot_in, cot_out, mix,
    hcols, lcols, cotg, gsend, grecv, counts, losses, total, loss_acc, coef,
    ld, w_send, w_recv, f_send, f_recv, b_send, b_recv, m_send, m_recv,
    h_send, h_recv, l_send, l_recv, c_send, c_recv, g_send, g_recv, k_send, k_recv,
    s_send, s_recv, t_send, t_recv,
):
    n_sec, samples, rank, prim, cuts = shape
    f32, bf16 = jnp.float32, jnp.bfloat16
    width = w.shape[0]
    out_width = head.shape[1]
    half = width // 2
    tang = samples * rank
    n_rows = tang + prim
    last = len(cuts) - 1
    shard = width // 4
    piece = shard // 2
    part = piece // PIECES
    cols = hcols.shape[1]
    dp = lax.axis_index("dp")
    sec = lax.axis_index("section")
    mp = lax.axis_index("mp")
    y, x = mp // 2, mp % 2
    is_first = sec == 0
    is_last = sec == n_sec - 1
    mps = (mp, 2 * y + (1 - x), 2 * (1 - y) + x, 2 * (1 - y) + (1 - x))
    dps = (dp, 1 - dp)
    peers = [(a, k) for a in range(2) for k in range(4) if (a, k) != (0, 0)]

    def plane(a, k):
        return (dps[a], sec, mps[k])

    barrier = pltpu.get_barrier_semaphore()
    for a, k in peers:
        pl.semaphore_signal(barrier, inc=1, device_id=plane(a, k), device_id_type=MESH)
    for hop in range(1, n_sec):
        other = (dp, (sec + hop) % n_sec, mp)
        pl.semaphore_signal(barrier, inc=1, device_id=other, device_id_type=MESH)

    own_rows = pl.ds(pl.multiple_of(mp * shard, shard), shard)
    load_w = pltpu.make_async_copy(shard_hbm, w.at[own_rows], ld.at[0])
    load_enc = pltpu.make_async_copy(enc_hbm, enc, ld.at[1])
    load_tan = pltpu.make_async_copy(tan_hbm, tan, ld.at[2])
    load_head = pltpu.make_async_copy(head_hbm, head, ld.at[3])
    load_tjac = pltpu.make_async_copy(tjac_hbm, tjac, ld.at[4])
    load_w.start()

    @pl.when(is_first)
    def _():
        load_enc.start()
        load_tan.start()

    @pl.when(is_last)
    def _():
        load_head.start()
        load_tjac.start()

    def remote(src, dst, send, recv, to):
        return pltpu.make_async_remote_copy(
            src_ref=src, dst_ref=dst, send_sem=send, recv_sem=recv,
            device_id=to, device_id_type=MESH,
        )

    def w_acts(s):
        def at(k):
            return pl.ds(pl.multiple_of(mps[k] * shard + dp * piece + s * part, part), part)

        lo, hi = pl.ds(0, half), pl.ds(half, half)
        acts = {
            "x": remote(w.at[at(0)], w.at[at(0)], w_send.at[s, 0], w_recv.at[s, 0], plane(0, 1)),
            "y": remote(w.at[at(0)], w.at[at(0)], w_send.at[s, 1], w_recv.at[s, 1], plane(0, 2)),
            "xy": remote(w.at[at(1), lo], w.at[at(1), lo], w_send.at[s, 2], w_recv.at[s, 2], plane(0, 2)),
            "yx": remote(w.at[at(2), hi], w.at[at(2), hi], w_send.at[s, 3], w_recv.at[s, 3], plane(0, 1)),
        }
        for k in range(1, 4):
            acts[k] = remote(w.at[at(k)], w.at[at(k)], w_send.at[s, 4 + k], w_recv.at[s, 4 + k], plane(1, 0))
        return acts

    def relay(acts):
        acts["x"].wait_recv()
        acts["xy"].start()
        acts[1].start()
        acts["y"].wait_recv()
        acts["yx"].start()
        acts[2].start()

    def close(acts):
        acts["xy"].wait_recv()
        acts["yx"].wait_recv()
        acts[3].start()

    def settle(acts, own):
        for k in range(0 if own else 1, 4):
            acts[k].wait_recv()
            acts[k].wait_send()
        for key in ("x", "y", "xy", "yx"):
            acts[key].wait_send()

    pl.semaphore_wait(barrier, len(peers) + n_sec - 1)
    load_w.wait()
    wg = [w_acts(s) for s in range(PIECES)]
    for acts in wg:
        acts["x"].start()
        acts["y"].start()

    def slot(index):
        return pl.ds(pl.multiple_of(index * 8, 8), 8)

    k_acts = [
        remote(counts.at[slot(0)], counts.at[slot(k)], k_send.at[k], k_recv.at[k], plane(0, k))
        for k in range(1, 4)
    ]
    per_batch = samples // MB
    place_of = dp * 4 + mp

    @pl.when(is_last)
    def _():
        mask = mask_ref[...].astype(f32)
        order = order_ref[...]
        lane = lax.broadcasted_iota(jnp.int32, (samples, LANES), 1)
        row = lax.broadcasted_iota(jnp.int32, (samples, LANES), 0)
        member = jnp.zeros((samples, LANES), f32)
        for p in range(samples):
            hit = (order[0:1, p : p + 1] == row) & (lane == p // per_batch)
            member = member + jnp.where(hit, 1.0, 0.0)
        weight = 1.0 + jnp.sum(mask, axis=1, keepdims=True)
        count = jnp.sum(member * weight, axis=0, keepdims=True)
        count = jnp.where(lane[0:1] < MB, count, 1.0)
        counts[pl.ds(0, 8), :] = jnp.broadcast_to(count, (8, LANES))
        for act in k_acts:
            act.start()
        tgt[...] = jnp.zeros_like(tgt)
        tgt[pl.ds(0, samples), :] = tgt_ref[...]
        loss_acc[...] = jnp.zeros_like(loss_acc)
        for act in k_acts:
            act.wait_recv()
            act.wait_send()
        summed = counts[pl.ds(0, 8), :]
        for k in range(1, 4):
            summed = summed + counts[pl.ds(8 * k, 8), :]
        scale = jnp.sum(member * (1.0 / summed[0:1]), axis=1, keepdims=True)
        coef[pl.ds(0, prim), :] = jnp.zeros((prim, LANES), f32)
        coef[pl.ds(0, samples), :] = jnp.broadcast_to(scale, (samples, LANES))
        eye = lax.broadcasted_iota(jnp.int32, (rank, rank), 0) == lax.broadcasted_iota(
            jnp.int32, (rank, rank), 1
        )
        for i in range(samples):
            picked = jnp.where(eye, jnp.broadcast_to(mask[i : i + 1], (rank, rank)), 0.0)
            column = jnp.sum(picked, axis=1, keepdims=True) * scale[i : i + 1]
            coef[pl.ds(prim + i * rank, rank), :] = jnp.broadcast_to(column, (rank, LANES))

    @pl.when(is_first)
    def _():
        inp[...] = jnp.zeros_like(inp)
        inp[pl.ds(0, samples), :] = inp_ref[...]
        load_enc.wait()
        load_tan.wait()
        for t in range(width // TILE):
            at = pl.ds(t * TILE, TILE)
            hin[pl.ds(0, prim), at] = jnp.dot(
                inp[...], enc[:, at], preferred_element_type=f32
            ).astype(bf16)
            hin[pl.ds(prim, tang), at] = jnp.dot(
                tan[...], enc[:, at], preferred_element_type=f32
            ).astype(bf16)

    sacc[...] = jnp.zeros_like(sacc)

    def flip(dst, src):
        block = 512

        @pl.loop(0, src.shape[0] // block)
        def _(r):
            for c in range(src.shape[1] // block):
                rows = pl.ds(pl.multiple_of(r * block, block), block)
                at = pl.ds(c * block, block)
                dst[at, rows] = src[rows, at].T

    @pl.when(is_last)
    def _():
        load_head.wait()
        load_tjac.wait()
        flip(headt, head)

    for acts in wg:
        relay(acts)
    for acts in wg:
        close(acts)
    for acts in wg:
        settle(acts, False)

    @pl.when(jnp.logical_not(is_first))
    def _():
        flip(wt, w)

    def f_rows(j):
        start, stop = cuts[j]
        return (0, stop + prim) if j == 0 else (start + prim, stop + prim)

    def b_rows(j):
        start, stop = cuts[j]
        return (start, tang + prim) if j == last else (start, stop)

    def span(ends):
        return pl.ds(ends[0], ends[1] - ends[0])

    def f_copy(j):
        return remote(
            hout.at[span(f_rows(j))], hin.at[span(f_rows(j))], f_send.at[j], f_recv.at[j],
            (dp, (sec + 1) % n_sec, mp),
        )

    def b_copy(j):
        return remote(
            cot_out.at[span(b_rows(j))], cot_in.at[span(b_rows(j))], b_send.at[j], b_recv.at[j],
            (dp, (sec + n_sec - 1) % n_sec, mp),
        )

    def pieces_of(start, stop):
        while start < stop:
            i = start // rank
            end = min(stop, (i + 1) * rank)
            yield i, start, end
            start = end

    def forward(j):
        start, stop = cuts[j]
        rows = span(f_rows(j))
        skip = prim if j == 0 else 0
        for t in range(width // TILE):
            at = pl.ds(t * TILE, TILE)
            act = jnp.dot(hin[rows, :], w[:, at], preferred_element_type=f32)
            if j == 0:
                top = pl.ds(0, prim)
                tanh_p = jnp.tanh(act[:prim])
                th[:, at] = tanh_p
                hout[top, at] = (hin[top, at].astype(f32) + tanh_p).astype(bf16)
            else:
                tanh_p = th[:, at]
            slope = 1.0 - tanh_p * tanh_p
            for i, lo, hi in pieces_of(start, stop):
                mine = act[skip + lo - start : skip + hi - start]
                pre[pl.ds(lo, hi - lo), at] = mine
                here = pl.ds(prim + lo, hi - lo)
                old = hin[here, at].astype(f32)
                hout[here, at] = (old + slope[i : i + 1] * mine).astype(bf16)

    def head_of(j):
        start, stop = cuts[j]
        ends = f_rows(j)
        rows = span(ends)
        first = 8 * ends[0]
        group = pl.ds(first, ends[1] - ends[0])
        scale = coef[rows, :][:, 0:1]
        for t in range(out_width // TILE):
            at = pl.ds(t * TILE, TILE)
            got = jnp.dot(hout[rows, :], head[:, at], preferred_element_type=f32)
            want = tjac[pl.ds(start, stop - start), at]
            if j == 0:
                want = jnp.concatenate([tgt[:, at], want], axis=0)
            miss = got - want.astype(f32)
            scaled = scale * miss
            cotg[group, at] = (2.0 * scaled).astype(bf16)
            loss_acc[...] += jnp.sum(scaled * miss, axis=0, keepdims=True)
        for t in range(width // TILE):
            at = pl.ds(t * TILE, TILE)
            back = jnp.dot(cotg[group, :], headt[:, at], preferred_element_type=f32).astype(bf16)
            if j == 0:
                cot_in[pl.ds(tang, prim), at] = back[:prim]
                cot_in[pl.ds(start, stop - start), at] = back[prim:]
            else:
                cot_in[pl.ds(start, stop - start), at] = back

    def backward(j):
        start, stop = cuts[j]
        ends = b_rows(j)
        base = 8 * ends[0]
        for t in range(width // TILE):
            at = pl.ds(t * TILE, TILE)
            tanh_p = th[:, at]
            slope = 1.0 - tanh_p * tanh_p
            for i, lo, hi in pieces_of(start, stop):
                cot = cot_in[pl.ds(lo, hi - lo), at].astype(f32)
                mix[pl.ds(base + lo - start, hi - lo), at] = (cot * slope[i : i + 1]).astype(bf16)
                sacc[pl.ds(i, 1), at] += jnp.sum(
                    cot * pre[pl.ds(lo, hi - lo), at], axis=0, keepdims=True
                )
            if j == last:
                cot = cot_in[pl.ds(tang, prim), at].astype(f32)
                top = cot * slope - 2.0 * sacc[:, at] * tanh_p * slope
                mix[pl.ds(base + stop - start, prim), at] = top.astype(bf16)

        @pl.when(sec > 0)
        def _():
            rows = pl.ds(base, ends[1] - ends[0])
            for t in range(width // TILE):
                at = pl.ds(t * TILE, TILE)
                back = jnp.dot(mix[rows, :], wt[:, at], preferred_element_type=f32)
                cot_out[span(ends), at] = (cot_in[span(ends), at].astype(f32) + back).astype(bf16)
            b_copy(j).start()

    def slot_copies(buf, send, recv, first, count, lanes):
        def at(a, k):
            return pl.ds(first + (a * 4 + k) * count, count)

        lo, hi = pl.ds(0, lanes // 2), pl.ds(lanes // 2, lanes // 2)
        acts = {
            "x": remote(buf.at[at(0, 0)], buf.at[at(0, 1)], send(0), recv(0), plane(0, 1)),
            "y": remote(buf.at[at(0, 0)], buf.at[at(0, 2)], send(1), recv(1), plane(0, 2)),
            "xy": remote(buf.at[at(0, 1), lo], buf.at[at(0, 3), lo], send(2), recv(2), plane(0, 2)),
            "yx": remote(buf.at[at(0, 2), hi], buf.at[at(0, 3), hi], send(3), recv(3), plane(0, 1)),
        }
        for k in range(4):
            acts[k] = remote(buf.at[at(0, k)], buf.at[at(1, k)], send(4 + k), recv(4 + k), plane(1, 0))
        return acts

    def open_slots(acts):
        acts["x"].start()
        acts["y"].start()
        acts[0].start()

    def mix_acts(j):
        start, stop = b_rows(j)
        return slot_copies(
            mix, lambda i: m_send.at[i, j], lambda i: m_recv.at[i, j], 8 * start, stop - start, width
        )

    def cotg_acts(j):
        start, stop = f_rows(j)
        return slot_copies(
            cotg, lambda i: c_send.at[i, j], lambda i: c_recv.at[i, j],
            8 * start, stop - start, out_width,
        )

    own_cols = pl.ds(pl.multiple_of(place_of * cols, cols), cols)

    def column_copies(src, rows, buf, first, stride, send, recv):
        acts = []
        for a, k in peers:
            at = a * 4 + k
            theirs = pl.ds(pl.multiple_of((dps[a] * 4 + mps[k]) * cols, cols), cols)
            acts.append(
                remote(
                    src.at[rows, theirs], buf.at[pl.ds(first + at * stride, rows.size)],
                    send.at[at], recv.at[at], plane(a, k),
                )
            )
        return acts

    def h_parts(j):
        start, stop = cuts[j]
        ends = b_rows(j)
        stride = ends[1] - ends[0]
        parts = [(j, pl.ds(prim + start, stop - start), 8 * ends[0], stride)]
        if j == last:
            parts.append((j + 1, pl.ds(0, prim), 8 * ends[0] + stop - start, stride))
        return parts

    def h_acts(j):
        acts = []
        for index, rows, first, stride in h_parts(j):
            acts += column_copies(
                hin, rows, hcols, first, stride, h_send.at[index], h_recv.at[index]
            )
        return acts

    def h_own(j):
        for _, rows, first, _ in h_parts(j):
            hcols[pl.ds(first, rows.size), :] = hin[rows, own_cols]

    def l_acts(j):
        start, stop = f_rows(j)
        return column_copies(
            hout, pl.ds(start, stop - start), lcols, 8 * start, stop - start,
            l_send.at[j], l_recv.at[j],
        )

    def grad(j):
        start, stop = b_rows(j)
        group = pl.ds(8 * start, 8 * (stop - start))
        for t in range(width // TILE):
            at = pl.ds(t * TILE, TILE)
            part = lax.dot_general(
                hcols[group, :], mix[group, at], (((0,), (0,)), ((), ())),
                preferred_element_type=f32,
            )
            if j == 0:
                dw_ref[:, at] = part
            else:
                dw_ref[:, at] += part

    def finish_mix(j):
        acts = mix_acts(j)
        close(acts)
        settle(acts, True)

    def finish_cols(j):
        for act in h_acts(j):
            act.wait_recv()
            act.wait_send()

    chunks = range(len(cuts))
    for j in chunks:
        @pl.when(jnp.logical_not(is_first))
        def _():
            f_copy(j).wait_recv()

        forward(j)

        @pl.when(jnp.logical_not(is_last))
        def _():
            f_copy(j).start()
            for act in h_acts(j):
                act.start()
            h_own(j)

        @pl.when(is_last)
        def _():
            head_of(j)
            open_slots(cotg_acts(j))
            for act in l_acts(j):
                act.start()
            backward(j)
            if j > 0:
                relay(cotg_acts(j - 1))
            start, stop = f_rows(j)
            lcols[pl.ds(8 * start, stop - start), :] = hout[pl.ds(start, stop - start), own_cols]

    @pl.when(is_last)
    def _():
        relay(cotg_acts(last))
        for j in chunks:
            open_slots(mix_acts(j))
        for j in chunks:
            for act in h_acts(j):
                act.start()
            h_own(j)
        mine = jnp.broadcast_to(jnp.sum(loss_acc[...], axis=1, keepdims=True), (8, LANES))
        losses[slot(place_of), :] = mine
        s_acts = [
            remote(
                losses.at[slot(place_of)], losses.at[slot(place_of)],
                s_send.at[a * 4 + k], s_recv.at[a * 4 + k], plane(a, k),
            )
            for a, k in peers
        ]
        for act in s_acts:
            act.start()
        for j in chunks:
            close(cotg_acts(j))
        for j in chunks:
            settle(cotg_acts(j), True)
            for act in l_acts(j):
                act.wait_recv()
                act.wait_send()
        share = out_width // n_sec
        for s in range(n_sec):
            got = lax.dot_general(
                lcols[...], cotg[:, s * share : (s + 1) * share], (((0,), (0,)), ((), ())),
                preferred_element_type=f32,
            )
            if s == n_sec - 1:
                gh_ref[...] = got
            else:
                gsend[s] = got.astype(bf16)
                remote(gsend.at[s], grecv, g_send.at[s], g_recv, (dp, s, mp)).start()
        for act in s_acts:
            act.wait_recv()
            act.wait_send()
        whole = losses[pl.ds(0, 8), :]
        for index in range(1, 8):
            whole = whole + losses[pl.ds(index * 8, 8), :]
        total[...] = whole
        for s in range(n_sec - 1):
            remote(total, total, t_send.at[s], t_recv, (dp, s, mp)).start()
        for j in chunks:
            relay(mix_acts(j))
        for j in chunks:
            finish_mix(j)
            finish_cols(j)
            grad(j)
        for s in range(n_sec - 1):
            remote(gsend.at[s], grecv, g_send.at[s], g_recv, (dp, s, mp)).wait_send()
            remote(total, total, t_send.at[s], t_recv, (dp, s, mp)).wait_send()

    @pl.when(jnp.logical_not(is_last))
    def _():
        for j in chunks:
            b_copy(j).wait_recv()
            backward(j)
            open_slots(mix_acts(j))
            if j > 0:
                relay(mix_acts(j - 1))
            if j > 1:
                finish_mix(j - 2)
                finish_cols(j - 2)
                grad(j - 2)
        relay(mix_acts(last))
        for j in (last - 1, last):
            if j >= 0:
                finish_mix(j)
                finish_cols(j)
                grad(j)
        remote(gsend.at[0], grecv, g_send.at[0], g_recv, (dp, sec + 1, mp)).wait_recv()
        gh_ref[...] = grecv[...].astype(f32)
        remote(total, total, t_send.at[0], t_recv, (dp, sec + 1, mp)).wait_recv()
        for j in chunks:
            f_copy(j).wait_send()

    @pl.when(jnp.logical_not(is_first))
    def _():
        for j in chunks:
            b_copy(j).wait_send()

    loss_ref[...] = total[...]


def fused(
    inputs, tangents, targets, target_jac, rank_mask, batch_order, encoder, layers, head_weight
):
    samples, rank = tangents.shape[:2]
    in_width = inputs.shape[1]
    width = layers.shape[2]
    out_width = head_weight.shape[1]
    n_sec = lax.axis_size("section")
    prim = -(-samples // SUBLANES) * SUBLANES
    tang = samples * rank
    n_rows = tang + prim
    cuts = cuts_of(tang)
    n = len(cuts)
    cols = width // (lax.axis_size("dp") * lax.axis_size("mp"))
    bf16, f32 = jnp.bfloat16, jnp.float32
    dma = pltpu.SemaphoreType.DMA
    vmem = pl.BlockSpec(memory_space=pltpu.VMEM)
    hbm = pl.BlockSpec(memory_space=pl.ANY)
    dw, gh, loss = pl.pallas_call(
        functools.partial(step_kernel, (n_sec, samples, rank, prim, cuts)),
        out_shape=(
            jax.ShapeDtypeStruct((cols, width), f32),
            jax.ShapeDtypeStruct((cols, out_width // n_sec), f32),
            jax.ShapeDtypeStruct((8, LANES), f32),
        ),
        in_specs=[hbm] * 5 + [vmem] * 4,
        out_specs=(vmem,) * 3,
        scratch_shapes=[
            pltpu.VMEM((width, width), bf16),
            pltpu.VMEM((width, width), bf16),
            pltpu.VMEM((in_width, width), bf16),
            pltpu.VMEM((width, out_width), bf16),
            pltpu.VMEM((out_width, width), bf16),
            pltpu.VMEM((tang, in_width), bf16),
            pltpu.VMEM((tang, out_width), bf16),
            pltpu.VMEM((prim, in_width), bf16),
            pltpu.VMEM((prim, out_width), bf16),
            pltpu.VMEM((n_rows, width), bf16),
            pltpu.VMEM((n_rows, width), bf16),
            pltpu.VMEM((tang, width), f32),
            pltpu.VMEM((prim, width), f32),
            pltpu.VMEM((prim, width), f32),
            pltpu.VMEM((n_rows, width), bf16),
            pltpu.VMEM((n_rows, width), bf16),
            pltpu.VMEM((8 * n_rows, width), bf16),
            pltpu.VMEM((8 * n_rows, cols), bf16),
            pltpu.VMEM((8 * n_rows, cols), bf16),
            pltpu.VMEM((8 * n_rows, out_width), bf16),
            pltpu.VMEM((n_sec - 1, cols, out_width // n_sec), bf16),
            pltpu.VMEM((cols, out_width // n_sec), bf16),
            pltpu.VMEM((32, LANES), f32),
            pltpu.VMEM((64, LANES), f32),
            pltpu.VMEM((8, LANES), f32),
            pltpu.VMEM((1, TILE), f32),
            pltpu.VMEM((n_rows, LANES), f32),
            dma((5,)), dma((PIECES, 8)), dma((PIECES, 8)),
            dma((n,)), dma((n,)), dma((n,)), dma((n,)),
            dma((8, n)), dma((8, n)),
            dma((n + 1, 8)), dma((n + 1, 8)), dma((n, 8)), dma((n, 8)),
            dma((8, n)), dma((8, n)),
            dma((n_sec,)), dma,
            dma((4,)), dma((4,)), dma((8,)), dma((8,)), dma((n_sec,)), dma,
        ],
        compiler_params=pltpu.CompilerParams(
            collective_id=0, has_side_effects=True, vmem_limit_bytes=62 * 2**20
        ),
    )(
        layers[0], encoder, head_weight, tangents.reshape(tang, in_width),
        target_jac.reshape(tang, out_width), inputs, targets, rank_mask, batch_order,
    )
    return (dw[None], gh, loss[0, 0] / (lax.axis_size("dp") * MB * out_width))


def solution(mesh):
    in_specs = (
        P(("dp", "mp"), None),
        P(("dp", "mp"), None, None),
        P(("dp", "mp"), None),
        P(("dp", "mp"), None, None),
        P(("dp", "mp"), None),
        P(("dp", "mp"), None),
        P(),
        P("section", "mp", None),
        P(),
    )
    out_specs = (P("section", ("dp", "mp"), None), P(("dp", "mp"), "section"), P())
    square_plane = mesh.shape["dp"] == 2 and mesh.shape["mp"] == 4
    body = fused if square_plane else local
    return jax.shard_map(body, mesh=mesh, in_specs=in_specs, out_specs=out_specs, check_vma=False)
```
